256 devices in a mesh: task: 8 (over y, core), param: 32 (over z, x).
Axes of the slice: x: 4, y: 4, z: 8, core: 2. Of those that a mesh axis runs over, the one named last changes fastest.
Arguments:
- params: bfloat16 [32, 2048, 4096], P('task', 'param'), may hold values from -6 to 6
- fisher: float32 [32, 2048, 4096], P('task', 'param'), may hold values from 3e-06 to 1, as said below
Outputs:
- merged: bfloat16 [2048, 4096], P('param')
The draws below stay inside these ranges and needn't reach their ends.
Inputs may be any that keep to these rules, and one draw needn't show every extreme that they name: `fisher`: every entry is positive; scales differ strongly between tasks and between regions of rows.
All inputs are finite; a program needn't handle non-finite values.
Results may differ from the reference program's by a relative error of at most 0.00045.
Values may be sent and summed in bfloat16 or wider, within the bound.
A program may use at most 64 MiB of HBM per device.

```python
import math
import jax
import jax.numpy as jnp
from jax import lax

FF = 4096
TASKS = 32
ROWS = 2048


def draw_fisher(key, part):
    first, second, third = jax.random.split(key, 3)
    region = jnp.exp(jax.random.uniform(first, (TASKS, 8), jnp.float32, math.log(1.0 / 256.0), 0.0))
    region = jnp.repeat(region, ROWS // 8, axis=1)
    base = jnp.exp(jax.random.uniform(second, (TASKS, ROWS, FF), jnp.float32, math.log(0.001), 0.0))
    return (base * region[:, :, None]).astype(jnp.float32)


def block_levels(own_key, dims, cuts, least, top_value):
    gain, own = 1.0, jax.random.fold_in(own_key, 6)
    for position, blocks in cuts:
        draws = jnp.exp(jax.random.uniform(jax.random.fold_in(own, position), (blocks,), jnp.float32, least / len(cuts), top_value / len(cuts)))
        gain = gain * jnp.repeat(draws, dims[position] // blocks).reshape([-1 if axis == position else 1 for axis in range(len(dims))])
    return gain


def scatter_about(own_key, dims, spread, bound, shards=(), kind=jnp.bfloat16):
    factor_of = block_levels(own_key, dims, shards, -0.22, 0.18) if shards else 1.0
    values = jax.random.normal(own_key, dims, jnp.float32) * spread * factor_of
    return jnp.minimum(jnp.maximum(values, -bound), bound).astype(kind)


def setup_inputs(seed: int = 0) -> dict:
    arg_keys = jax.random.split(jax.random.key(seed), 3)
    return {
        "params": scatter_about(arg_keys[0], (TASKS, ROWS, FF), 1.0, 6.0, ((0, 8), (1, 32))),
        "fisher": draw_fisher(jax.random.fold_in(arg_keys[2], 71), 0),
    }


def reference(params, fisher):
    peak = jnp.max(fisher, axis=(1, 2))
    total = jnp.sum(fisher, axis=(1, 2))
    count = float(ROWS * FF)
    factor = count * peak / total

    def one_task(carry, items):
        theta, info, top, mult = items
        weight = jnp.clip(info / top, 0.002, 0.25) * mult
        return (carry[0] + weight * theta.astype(jnp.float32), carry[1] + weight), None

    start = (jnp.zeros((ROWS, FF), jnp.float32), jnp.zeros((ROWS, FF), jnp.float32))
    sums, unused = lax.scan(one_task, start, (params, fisher, peak, factor))
    return (sums[0] / sums[1]).astype(jnp.bfloat16)
```

```python
import functools

import jax
import jax.numpy as jnp
from jax import lax
from jax.experimental import pallas as pl
from jax.experimental.pallas import tpu as pltpu
from jax.sharding import PartitionSpec as P

F32, BF16 = jnp.float32, jnp.bfloat16
MESH = pl.DeviceIdType.MESH
X, Y, Z, CORES = 4, 4, 8, 2
TASKS, ROWS, COLS = 4, 64, 4096
HALF = ROWS // CORES
CHUNK = COLS // Y
PIECES = 4
WIDE = CHUNK // PIECES
COUNT = float(ROWS * X * Z * COLS)
LEAST, MOST = 0.002, 0.25


def remote(src, dst, send, recv, where):
    return pltpu.make_async_remote_copy(
        src_ref=src, dst_ref=dst, send_sem=send, recv_sem=recv, device_id=where, device_id_type=MESH
    )


def kernel(
    params, fisher, out, fi, fo, pa, near, far, sa, sc, sb, so, ra, rc, rb,
    load_f, load_p, swap_f, swap_p, near_s, near_r, far_s, far_r,
    a_s, a_r, b_s, b_r, c_s, c_r, ag_s, ag_r, fw_s, fw_r,
):
    task, place = lax.axis_index("task"), lax.axis_index("param")
    core, y = lax.rem(task, CORES), lax.div(task, CORES)
    x, z = lax.rem(place, X), lax.div(place, X)
    other = 1 - core

    def at_xc(dx, dc):
        c = core if dc == 0 else other
        return (y * CORES + c, z * X + lax.rem(x + dx, X))

    def at_z(dz):
        return (task, lax.rem(z + dz, Z) * X + x)

    def at_y(dy):
        return (lax.rem(y + dy, Y) * CORES + core, place)

    partner = (y * CORES + other, place)
    nears = [(dx, dc) for dx in range(X) for dc in range(CORES) if dx or dc]

    barrier = pltpu.get_barrier_semaphore()
    peers = [at_z(dz) for dz in (4, 3, 5, 2, 6, 1, 7)] + [at_xc(*n) for n in nears] + [at_y(dy) for dy in (2, 1, 3)]
    for peer in peers:
        pl.semaphore_signal(barrier, inc=1, device_id=peer, device_id_type=MESH)

    mine = pl.ds(pl.multiple_of(core * HALF, HALF), HALF)
    yours = pl.ds(pl.multiple_of(other * HALF, HALF), HALF)
    loads = []
    for t in range(TASKS):
        for half, (rows, dst) in enumerate(((yours, fo.at[t]), (mine, fi.at[t]))):
            copy = pltpu.make_async_copy(fisher.at[t, rows, :], dst, load_f.at[t, half])
            copy.start()
            loads.append(copy)
    loads_p = []
    for t in range(TASKS):
        copy = pltpu.make_async_copy(params.at[t, mine, :], pa.at[t], load_p.at[t])
        copy.start()
        loads_p.append(copy)

    lane = lax.broadcasted_iota(jnp.int32, (1, 128), 1)
    row = jnp.zeros((1, 128), F32)

    def stats(ref, t, carry):
        def step(k, c):
            v = ref[t, :, pl.ds(pl.multiple_of(k * 128, 128), 128)]
            return jnp.maximum(c[0], v), c[1] + v

        return lax.fori_loop(0, COLS // 128, step, carry, unroll=8)

    for t in range(TASKS):
        carry = (jnp.zeros((HALF, 128), F32), jnp.zeros((HALF, 128), F32))
        loads[2 * t].wait()
        carry = stats(fo, t, carry)
        loads[2 * t + 1].wait()
        top, tot = stats(fi, t, carry)
        top = jnp.max(jnp.max(top, axis=0, keepdims=True), axis=1, keepdims=True)
        tot = jnp.sum(jnp.sum(tot, axis=0, keepdims=True), axis=1, keepdims=True)
        row = jnp.where(lane == core * TASKS + t, top, row)
        row = jnp.where(lane == 8 + core * TASKS + t, tot, row)
    near[0] = row

    pl.semaphore_wait(barrier, len(peers))

    near_copies = []
    for i, (dx, dc) in enumerate(nears):
        slot = dx * CORES + dc
        copy = remote(near.at[0], near.at[slot], near_s.at[slot], near_r.at[slot], at_xc(dx, dc))
        copy.start()
        near_copies.append(copy)
    swaps = []
    for t in range(TASKS):
        copy = remote(fo.at[t], fi.at[TASKS + t], swap_f.at[0, t], swap_f.at[1, t], partner)
        copy.start()
        swaps.append(copy)
    for t in range(TASKS):
        copy = remote(params.at[t, yours, :], pa.at[TASKS + t], swap_p.at[0, t], swap_p.at[1, t], partner)
        copy.start()
        swaps.append(copy)

    def combined(ref, n):
        top, tot = ref[0], ref[0]
        for i in range(1, n):
            top, tot = jnp.maximum(top, ref[i]), tot + ref[i]
        return jnp.where(lane < 8, top, tot)

    for copy in near_copies:
        copy.wait_recv()
    far[0] = combined(near, X * CORES)
    far_copies = []
    for dz in (4, 3, 5, 2, 6, 1, 7):
        copy = remote(far.at[0], far.at[dz], far_s.at[dz], far_r.at[dz], at_z(dz))
        copy.start()
        far_copies.append(copy)
    for copy in loads_p:
        copy.wait()
    for copy in swaps:
        copy.wait_recv()
    for copy in far_copies:
        copy.wait_recv()
    row = combined(far, Z)
    scale_row = COUNT / row
    scale, low, high = [], [], []
    for t in range(2 * TASKS):
        at = (core if t < TASKS else other) * TASKS + t % TASKS
        top = jnp.sum(jnp.where(lane == at, row, 0.0))
        s = jnp.sum(jnp.where(lane == 8 + at, scale_row, 0.0))
        scale.append(s)
        low.append(LEAST * top * s)
        high.append(MOST * top * s)

    def partial(chunk, p, dst):
        cols = pl.ds(pl.multiple_of(chunk * CHUNK + p * WIDE, WIDE), WIDE)
        numer = denom = jnp.zeros((HALF, WIDE), F32)
        for t in range(2 * TASKS):
            w = jnp.minimum(jnp.maximum(fi[t, :, cols] * scale[t], low[t]), high[t])
            denom = denom + w
            numer = numer + w * pa[t, :, cols].astype(F32)
        dst[p, 0] = numer
        dst[p, 1] = denom

    step = 2 * core - 1
    ahead, behind, across = lax.rem(y + step + Y, Y), lax.rem(y - step + Y, Y), lax.rem(y + 2, Y)
    to_ahead, to_behind = (ahead * CORES + core, place), (behind * CORES + core, place)
    copies_a, copies_b, copies_c = [], [], []
    for p in range(PIECES):
        partial(across, p, sa)
        copies_a.append(remote(sa.at[p], ra.at[p], a_s.at[p], a_r.at[p], to_ahead))
        copies_a[p].start()
        partial(behind, p, sc)
        copies_c.append(remote(sc.at[p], rc.at[p], c_s.at[p], c_r.at[p], to_behind))
        copies_c[p].start()
    for p in range(PIECES):
        partial(ahead, p, sb)
    for p in range(PIECES):
        partial(y, p, so)
    for p in range(PIECES):
        copies_a[p].wait_recv()
        sb[p] = sb[p] + ra[p]
        copies_b.append(remote(sb.at[p], rb.at[p], b_s.at[p], b_r.at[p], to_ahead))
        copies_b[p].start()

    def block(chunk, p):
        return out.at[mine, pl.ds(pl.multiple_of(chunk * CHUNK + p * WIDE, WIDE), WIDE)]

    gathers, forwards = {}, {}

    def finish(p):
        copies_c[p].wait_recv()
        copies_b[p].wait_recv()
        total = so[p] + rc[p] + rb[p]
        here = block(y, p)
        here[...] = (total[0] / total[1]).astype(BF16)
        for dy in (2, 1, 3):
            gathers[p, dy] = remote(here, here, ag_s.at[p, dy], ag_r.at[p, dy], at_y(dy))
            gathers[p, dy].start()
        forwards[p, 0] = remote(here, here, fw_s.at[p, 0], fw_r.at[p, 0], partner)
        forwards[p, 0].start()

    def forward(p):
        for dy in (1, 3, 2):
            gathers[p, dy].wait_recv()
            there = block(lax.rem(y - dy + Y, Y), p)
            forwards[p, dy] = remote(there, there, fw_s.at[p, dy], fw_r.at[p, dy], partner)
            forwards[p, dy].start()

    for p in range(PIECES):
        finish(p)
        if p >= 2:
            forward(p - 2)
    forward(PIECES - 2)
    forward(PIECES - 1)

    for copy in near_copies + far_copies + swaps + copies_a + copies_b + copies_c + list(gathers.values()):
        copy.wait_send()
    for copy in forwards.values():
        copy.wait()


def local(params, fisher):
    dma = pltpu.SemaphoreType.DMA
    pieces = pltpu.VMEM((PIECES, 2, HALF, WIDE), F32)
    return pl.pallas_call(
        kernel,
        out_shape=jax.ShapeDtypeStruct((ROWS, COLS), BF16),
        in_specs=[pl.BlockSpec(memory_space=pl.ANY)] * 2,
        out_specs=pl.BlockSpec(memory_space=pltpu.VMEM),
        scratch_shapes=[
            pltpu.VMEM((2 * TASKS, HALF, COLS), F32),
            pltpu.VMEM((TASKS, HALF, COLS), F32),
            pltpu.VMEM((2 * TASKS, HALF, COLS), BF16),
            pltpu.VMEM((X * CORES, 1, 128), F32),
            pltpu.VMEM((Z, 1, 128), F32),
            *[pieces] * 7,
            dma((TASKS, 2)), dma((TASKS,)), dma((2, TASKS)), dma((2, TASKS)),
            *[dma((8,))] * 4,
            *[dma((PIECES,))] * 6,
            *[dma((PIECES, Y))] * 4,
        ],
        compiler_params=pltpu.CompilerParams(collective_id=0, has_side_effects=True),
        name="merge",
    )(params, fisher)


def solution(mesh):
    in_specs = (P("task", "param", None), P("task", "param", None))
    return jax.shard_map(local, mesh=mesh, in_specs=in_specs, out_specs=P("param", None), check_vma=False)
```

```python
import functools

import jax
import jax.numpy as jnp
from jax import lax
from jax.experimental import pallas as pl
from jax.experimental.pallas import tpu as pltpu
from jax.sharding import PartitionSpec as P

F32, BF16 = jnp.float32, jnp.bfloat16
MESH = pl.DeviceIdType.MESH
X, Y, Z, CORES = 4, 4, 8, 2
TASKS, ROWS, COLS = 4, 64, 4096
HALF = ROWS // CORES
CHUNK = COLS // Y
PIECES = 4
WIDE = CHUNK // PIECES
COUNT = float(ROWS * X * Z * COLS)
LEAST, MOST = 0.002, 0.25


def remote(src, dst, send, recv, where):
    return pltpu.make_async_remote_copy(
        src_ref=src, dst_ref=dst, send_sem=send, recv_sem=recv, device_id=where, device_id_type=MESH
    )


def kernel(
    params, fisher, out, fi, fo, pa, near, far, sa, sc, sb, so, ra, rc, rb,
    load_f, load_p, swap_f, swap_p, near_s, near_r, far_s, far_r,
    a_s, a_r, b_s, b_r, c_s, c_r, ag_s, ag_r, fw_s, fw_r,
):
    task, place = lax.axis_index("task"), lax.axis_index("param")
    core, y = lax.rem(task, CORES), lax.div(task, CORES)
    x, z = lax.rem(place, X), lax.div(place, X)
    other = 1 - core

    def at_xc(dx, dc):
        c = core if dc == 0 else other
        return (y * CORES + c, z * X + lax.rem(x + dx, X))

    def at_z(dz):
        return (task, lax.rem(z + dz, Z) * X + x)

    def at_y(dy):
        return (lax.rem(y + dy, Y) * CORES + core, place)

    partner = (y * CORES + other, place)
    nears = [(dx, dc) for dx in range(X) for dc in range(CORES) if dx or dc]

    barrier = pltpu.get_barrier_semaphore()
    peers = [at_z(dz) for dz in (4, 3, 5, 2, 6, 1, 7)] + [at_xc(*n) for n in nears] + [at_y(dy) for dy in (2, 1, 3)]
    for peer in peers:
        pl.semaphore_signal(barrier, inc=1, device_id=peer, device_id_type=MESH)

    mine = pl.ds(pl.multiple_of(core * HALF, HALF), HALF)
    yours = pl.ds(pl.multiple_of(other * HALF, HALF), HALF)
    loads = []
    for t in range(TASKS):
        for half, (rows, dst) in enumerate(((yours, fo.at[t]), (mine, fi.at[t]))):
            copy = pltpu.make_async_copy(fisher.at[t, rows, :], dst, load_f.at[t, half])
            copy.start()
            loads.append(copy)
    loads_p = []
    for t in range(TASKS):
        copy = pltpu.make_async_copy(params.at[t, mine, :], pa.at[t], load_p.at[t])
        copy.start()
        loads_p.append(copy)

    lane = lax.broadcasted_iota(jnp.int32, (1, 128), 1)
    row = jnp.zeros((1, 128), F32)

    def stats(ref, t, carry):
        def step(k, c):
            v = ref[t, :, pl.ds(pl.multiple_of(k * 128, 128), 128)]
            return jnp.maximum(c[0], v), c[1] + v

        return lax.fori_loop(0, COLS // 128, step, carry, unroll=8)

    for t in range(TASKS):
        carry = (jnp.zeros((HALF, 128), F32), jnp.zeros((HALF, 128), F32))
        loads[2 * t].wait()
        carry = stats(fo, t, carry)
        loads[2 * t + 1].wait()
        top, tot = stats(fi, t, carry)
        top = jnp.max(jnp.max(top, axis=0, keepdims=True), axis=1, keepdims=True)
        tot = jnp.sum(jnp.sum(tot, axis=0, keepdims=True), axis=1, keepdims=True)
        row = jnp.where(lane == core * TASKS + t, top, row)
        row = jnp.where(lane == 8 + core * TASKS + t, tot, row)
    near[0] = row

    pl.semaphore_wait(barrier, len(peers))

    near_copies = []
    for i, (dx, dc) in enumerate(nears):
        slot = dx * CORES + dc
        copy = remote(near.at[0], near.at[slot], near_s.at[slot], near_r.at[slot], at_xc(dx, dc))
        copy.start()
        near_copies.append(copy)
    swaps = []
    for t in range(TASKS):
        copy = remote(fo.at[t], fi.at[TASKS + t], swap_f.at[0, t], swap_f.at[1, t], partner)
        copy.start()
        swaps.append(copy)
    for t in range(TASKS):
        copy = remote(params.at[t, yours, :], pa.at[TASKS + t], swap_p.at[0, t], swap_p.at[1, t], partner)
        copy.start()
        swaps.append(copy)

    def combined(ref, n):
        top, tot = ref[0], ref[0]
        for i in range(1, n):
            top, tot = jnp.maximum(top, ref[i]), tot + ref[i]
        return jnp.where(lane < 8, top, tot)

    for copy in near_copies:
        copy.wait_recv()
    far[0] = combined(near, X * CORES)
    far_copies = []
    for dz in (4, 3, 5, 2, 6, 1, 7):
        copy = remote(far.at[0], far.at[dz], far_s.at[dz], far_r.at[dz], at_z(dz))
        copy.start()
        far_copies.append(copy)
    for copy in loads_p:
        copy.wait()
    for copy in swaps:
        copy.wait_recv()
    for copy in far_copies:
        copy.wait_recv()
    row = combined(far, Z)
    scale_row = COUNT / row
    scale, low, high = [], [], []
    for t in range(2 * TASKS):
        at = (core if t < TASKS else other) * TASKS + t % TASKS
        top = jnp.sum(jnp.where(lane == at, row, 0.0))
        s = jnp.sum(jnp.where(lane == 8 + at, scale_row, 0.0))
        scale.append(s)
        low.append(LEAST * top * s)
        high.append(MOST * top * s)

    def partial(chunk, p, dst):
        cols = pl.ds(pl.multiple_of(chunk * CHUNK + p * WIDE, WIDE), WIDE)
        numer = denom = jnp.zeros((HALF, WIDE), F32)
        for t in range(2 * TASKS):
            w = jnp.minimum(jnp.maximum(fi[t, :, cols] * scale[t], low[t]), high[t])
            denom = denom + w
            numer = numer + w * pa[t, :, cols].astype(F32)
        dst[p, 0] = numer
        dst[p, 1] = denom

    step = 2 * core - 1
    ahead, behind, across = lax.rem(y + step + Y, Y), lax.rem(y - step + Y, Y), lax.rem(y + 2, Y)
    to_ahead, to_behind = (ahead * CORES + core, place), (behind * CORES + core, place)
    copies_a, copies_b, copies_c = [], [], []
    for p in range(PIECES):
        partial(across, p, sa)
        copies_a.append(remote(sa.at[p], ra.at[p], a_s.at[p], a_r.at[p], to_ahead))
        copies_a[p].start()
        partial(behind, p, sc)
        copies_c.append(remote(sc.at[p], rc.at[p], c_s.at[p], c_r.at[p], to_behind))
        copies_c[p].start()
    for p in range(PIECES):
        partial(ahead, p, sb)
    for p in range(PIECES):
        partial(y, p, so)
    for p in range(PIECES):
        copies_a[p].wait_recv()
        sb[p] = sb[p] + ra[p]
        copies_b.append(remote(sb.at[p], rb.at[p], b_s.at[p], b_r.at[p], to_ahead))
        copies_b[p].start()

    def block(chunk, p):
        return out.at[mine, pl.ds(pl.multiple_of(chunk * CHUNK + p * WIDE, WIDE), WIDE)]

    gathers, forwards = {}, {}

    def finish(p):
        copies_c[p].wait_recv()
        copies_b[p].wait_recv()
        total = so[p] + rc[p] + rb[p]
        here = block(y, p)
        here[...] = (total[0] / total[1]).astype(BF16)
        for dy in (2, 1, 3):
            gathers[p, dy] = remote(here, here, ag_s.at[p, dy], ag_r.at[p, dy], at_y(dy))
            gathers[p, dy].start()
        forwards[p, 0] = remote(here, here, fw_s.at[p, 0], fw_r.at[p, 0], partner)
        forwards[p, 0].start()

    def forward(p):
        for dy in (1, 3, 2):
            gathers[p, dy].wait_recv()
            there = block(lax.rem(y - dy + Y, Y), p)
            forwards[p, dy] = remote(there, there, fw_s.at[p, dy], fw_r.at[p, dy], partner)
            forwards[p, dy].start()

    for p in range(PIECES):
        finish(p)
        if p >= 2:
            forward(p - 2)
    forward(PIECES - 2)
    forward(PIECES - 1)

    for copy in near_copies + far_copies + swaps + copies_a + copies_b + copies_c + list(gathers.values()):
        copy.wait_send()
    for copy in forwards.values():
        copy.wait()


def local(params, fisher):
    dma = pltpu.SemaphoreType.DMA
    pieces = pltpu.VMEM((PIECES, 2, HALF, WIDE), F32)
    return pl.pallas_call(
        kernel,
        out_shape=pltpu.VMEM((ROWS, COLS), BF16),
        in_specs=[pl.BlockSpec(memory_space=pl.ANY)] * 2,
        out_specs=pl.BlockSpec(memory_space=pltpu.VMEM),
        scratch_shapes=[
            pltpu.VMEM((2 * TASKS, HALF, COLS), F32),
            pltpu.VMEM((TASKS, HALF, COLS), F32),
            pltpu.VMEM((2 * TASKS, HALF, COLS), BF16),
            pltpu.VMEM((X * CORES, 1, 128), F32),
            pltpu.VMEM((Z, 1, 128), F32),
            *[pieces] * 7,
            dma((TASKS, 2)), dma((TASKS,)), dma((2, TASKS)), dma((2, TASKS)),
            *[dma((8,))] * 4,
            *[dma((PIECES,))] * 6,
            *[dma((PIECES, Y))] * 4,
        ],
        compiler_params=pltpu.CompilerParams(collective_id=0, has_side_effects=True),
        name="merge",
    )(params, fisher)


def solution(mesh):
    in_specs = (P("task", "param", None), P("task", "param", None))
    return jax.shard_map(local, mesh=mesh, in_specs=in_specs, out_specs=P("param", None), check_vma=False)
```
